32 devices in a mesh: seq: 8 (over y, x, core), head: 4 (over z).
Axes of the slice: x: 2, y: 2, z: 4, core: 2. Of those that a mesh axis runs over, the one named last changes fastest.
Arguments:
- latent: bfloat16 [1024, 1024], P('seq'), may hold values from -15 to 15
- probe: bfloat16 [1024, 1024], P('seq'), may hold values from -6 to 6
- time_embed: float32 [1024], replicated, may hold values from -6 to 6
- gain_attn: float32 [1024], replicated, may hold values from 0.1 to 1.9
- w_query: bfloat16 [1024, 1024], P(None, 'head'), may hold values from -0.625 to 0.625
- w_key: bfloat16 [1024, 1024], P(None, 'head'), may hold values from -11 to 11
- w_value: bfloat16 [1024, 1024], P(None, 'head'), may hold values from -0.1875 to 0.1875
- w_out: bfloat16 [1024, 1024], P('head'), may hold values from -0.1875 to 0.1875
- gain_mlp: float32 [1024], replicated, may hold values from 0.1 to 1.9
- w_in: bfloat16 [1024, 4096], P(None, 'head'), may hold values from -0.1875 to 0.1875
- w_down: bfloat16 [4096, 1024], P('head'), may hold values from -0.09375 to 0.09375
Outputs:
- latent_end: float32 [1024, 1024], P('seq')
- frame_trace: float32 [1024], P('seq')
- frame_logp: float32 [1024], P('seq')
- mean_logp: float32 [], replicated
The draws below stay inside these ranges and needn't reach their ends.
All inputs are finite; a program needn't handle non-finite values.
Results may differ from the reference program's by a relative error of at most 0.03.
The reference program's roundings to bfloat16 on the way count: a program that leaves them out, or rounds other values in their place, can miss the bound.
Values may be sent and summed in bfloat16 or wider, within the bound.
A program may use at most 64 MiB of HBM per device.

```python
import math
import jax
import jax.numpy as jnp
from jax import lax

D = 1024
HEADS = 16
HEAD_DIM = 64
FF = 4096
STEPS = 2
FRAMES = 1024


def weight_pair(key):
    base = jax.random.fold_in(key, 11)
    first, second = jax.random.split(base, 2)
    query_weight = jnp.clip(jax.random.normal(first, (D, D), jnp.float32), -5.0, 5.0) * D ** (-0.5)
    noise = jnp.clip(jax.random.normal(second, (D, D), jnp.float32), -5.0, 5.0) * D ** (-0.5)
    key_weight = 3.0 * noise
    return (query_weight, key_weight)


def draw_w_query(key, part):
    return weight_pair(key)[0].astype(jnp.bfloat16)


def draw_w_key(key, part):
    return weight_pair(key)[1].astype(jnp.bfloat16)


def draw_latent(key, part):
    base = jax.random.fold_in(key, 23)
    position = jnp.arange(FRAMES, dtype=jnp.float32) / max(FRAMES - 1, 1)
    entries = jnp.clip(jax.random.normal(base, (FRAMES, D), jnp.float32), -5.0, 5.0)
    ramp = 1.0 + 2.0 * position
    return (entries * ramp[:, None]).astype(jnp.bfloat16)


def steps_of(key, extent, shards, low, high):
    factor_of, own = 1.0, jax.random.fold_in(key, 6)
    for dim, blocks in shards:
        heights = jnp.exp(jax.random.uniform(jax.random.fold_in(own, dim), (blocks,), jnp.float32, low / len(shards), high / len(shards)))
        factor_of = factor_of * jnp.repeat(heights, extent[dim] // blocks).reshape([-1 if axis == dim else 1 for axis in range(len(extent))])
    return factor_of


def normal_values(stream_key, extent, deviation, most, shards=(), held_as=jnp.bfloat16):
    array = jax.random.normal(stream_key, extent, jnp.float32) * deviation
    if len(shards) > 0:
        array = steps_of(stream_key, extent, shards, -0.22, 0.18) * array
    return jnp.clip(array, min=-most, max=most).astype(held_as)


def setup_inputs(seed: int = 0) -> dict:
    key_of = jax.random.split(jax.random.key(seed), 12)
    latent = draw_latent(jax.random.fold_in(key_of[11], 71), 0)
    probe = normal_values(key_of[1], (FRAMES, D), 1.0, 6.0, ((0, 8),))
    time_embed = normal_values(key_of[2], (D,), 1.0, 6.0, (), jnp.float32)
    gain_attn = jnp.clip(1.0 + 0.18 * jax.random.normal(key_of[3], (D,), jnp.float32), 0.1, 1.9)
    w_query = draw_w_query(jax.random.fold_in(key_of[11], 71), 0)
    w_key = draw_w_key(jax.random.fold_in(key_of[11], 71), 0)
    w_value = normal_values(key_of[6], (D, D), D ** -0.5, 0.1875, ((1, 4),))
    w_out = normal_values(key_of[7], (D, D), D ** -0.5, 0.1875, ((0, 4),))
    gain_mlp = jnp.clip(1.0 + 0.18 * jax.random.normal(key_of[8], (D,), jnp.float32), 0.1, 1.9)
    w_in = normal_values(key_of[9], (D, FF), D ** -0.5, 0.1875, ((1, 4),))
    w_down = normal_values(key_of[10], (FF, D), FF ** -0.5, 0.09375, ((0, 4),))
    return dict(latent=latent, probe=probe, time_embed=time_embed, gain_attn=gain_attn, w_query=w_query, w_key=w_key, w_value=w_value, w_out=w_out, gain_mlp=gain_mlp, w_in=w_in, w_down=w_down)


EPSILON = 1e-05
GELU_COEF = 0.044715
ROOT_TWO_PI = math.sqrt(2.0 / math.pi)

def norm_pair(values, tangent, norm_gain):
    meansq = lax.optimization_barrier(jnp.mean(values * values, axis=-1, keepdims=True)) + EPSILON
    inverse = lax.rsqrt(meansq)
    inner_mean = lax.optimization_barrier(jnp.mean(values * tangent, axis=-1, keepdims=True))
    primal = values * inverse * norm_gain
    derived = (tangent * inverse - values * inverse ** 3 * inner_mean) * norm_gain
    return (primal.astype(jnp.bfloat16), derived.astype(jnp.bfloat16))

def gelu_pair(pre_act, tangent):
    cubic_arg = pre_act + GELU_COEF * pre_act ** 3
    tanh_value = jnp.tanh(ROOT_TWO_PI * cubic_arg)
    output = 0.5 * pre_act * (1.0 + tanh_value)
    slope_value = 0.5 * (1.0 + tanh_value) + 0.5 * pre_act * (1.0 - tanh_value * tanh_value) * ROOT_TWO_PI * (1.0 + 3.0 * GELU_COEF * pre_act * pre_act)
    return (output.astype(jnp.bfloat16), (slope_value * tangent).astype(jnp.bfloat16))

def attention(queries, query_tang, keys, vals, key_tang, val_tang):
    scale = HEAD_DIM ** (-0.5)

    def heads_of(matrix):
        return matrix.astype(jnp.float32).reshape(FRAMES, HEADS, HEAD_DIM)
    keys_all = heads_of(keys)
    vals_all = heads_of(vals)
    key_tang_all = heads_of(key_tang)
    val_tang_all = heads_of(val_tang)
    block = math.gcd(FRAMES, 512)

    def one_block(pair):
        block_queries, block_tang = pair
        scores = jnp.einsum('bhd,shd->hbs', block_queries, keys_all) * scale
        score_tang = (jnp.einsum('bhd,shd->hbs', block_tang, keys_all) + jnp.einsum('bhd,shd->hbs', block_queries, key_tang_all)) * scale
        row_top = lax.optimization_barrier(jnp.max(scores, axis=-1, keepdims=True))
        weights = jnp.exp(scores - row_top)
        total = lax.optimization_barrier(jnp.sum(weights, axis=-1))
        weighted = weights * score_tang
        carried = lax.optimization_barrier(jnp.sum(weighted, axis=-1))
        rounded = lax.optimization_barrier(weights.astype(jnp.bfloat16)).astype(jnp.float32)
        rounded_tang = lax.optimization_barrier(weighted.astype(jnp.bfloat16)).astype(jnp.float32)
        acc_primal = jnp.einsum('hbs,shd->bhd', rounded, vals_all)
        acc_tang = jnp.einsum('hbs,shd->bhd', rounded_tang, vals_all) + jnp.einsum('hbs,shd->bhd', rounded, val_tang_all)
        total_t = jnp.transpose(total)[:, :, None]
        carried_t = jnp.transpose(carried)[:, :, None]
        primal = acc_primal / total_t
        tangent = acc_tang / total_t - carried_t / total_t * primal
        return (primal.astype(jnp.bfloat16), tangent.astype(jnp.bfloat16))
    query_blocks = heads_of(queries).reshape(FRAMES // block, block, HEADS, HEAD_DIM)
    tang_blocks = heads_of(query_tang).reshape(FRAMES // block, block, HEADS, HEAD_DIM)
    head_out, head_tang = lax.map(one_block, (query_blocks, tang_blocks))
    return (head_out.reshape(FRAMES, D), head_tang.reshape(FRAMES, D))

def vector_field(inputs, direction, gain_attn, w_query, w_key, w_value, w_out, gain_mlp, w_in, w_down):
    normed, normed_tang = norm_pair(inputs, direction, gain_attn)

    def project(weight):
        primal = jnp.dot(normed, weight, preferred_element_type=jnp.float32).astype(jnp.bfloat16)
        tangent = jnp.dot(normed_tang, weight, preferred_element_type=jnp.float32).astype(jnp.bfloat16)
        return (primal, tangent)
    queries, query_tang = project(w_query)
    keys, key_tang = project(w_key)
    vals, val_tang = project(w_value)
    head_out, head_tang = attention(queries, query_tang, keys, vals, key_tang, val_tang)
    attn = jnp.dot(head_out, w_out, preferred_element_type=jnp.float32)
    attn_tang = jnp.dot(head_tang, w_out, preferred_element_type=jnp.float32)
    middle = inputs + attn
    middle_tang = direction + attn_tang
    normed_mlp, normed_mlp_tang = norm_pair(middle, middle_tang, gain_mlp)
    pre_act = jnp.dot(normed_mlp, w_in, preferred_element_type=jnp.float32)
    pre_tang = jnp.dot(normed_mlp_tang, w_in, preferred_element_type=jnp.float32)
    activ, activ_tang = gelu_pair(pre_act, pre_tang)
    mlp_out = jnp.dot(activ, w_down, preferred_element_type=jnp.float32)
    mlp_tang = jnp.dot(activ_tang, w_down, preferred_element_type=jnp.float32)
    return (attn + mlp_out, attn_tang + mlp_tang)

def reference(latent, probe, time_embed, gain_attn, w_query, w_key, w_value, w_out, gain_mlp, w_in, w_down):
    state = latent.astype(jnp.float32)
    direction = probe.astype(jnp.float32)
    trace = jnp.zeros((FRAMES,), jnp.float32)
    for euler_step in range(STEPS):
        inputs = state + euler_step / STEPS * time_embed
        field, field_tang = vector_field(inputs, direction, gain_attn, w_query, w_key, w_value, w_out, gain_mlp, w_in, w_down)
        trace = trace + lax.optimization_barrier(jnp.sum(direction * field_tang, axis=-1)) / (STEPS * D)
        state = state + field / STEPS
    frame_logp = trace - 0.5 * lax.optimization_barrier(jnp.sum(state * state, axis=-1)) / D - 0.5 * math.log(2.0 * math.pi)
    mean_logp = jnp.mean(frame_logp)
    return (state, trace, frame_logp, mean_logp)
```

```python
import functools
import math

import jax
import jax.numpy as jnp
from jax import lax
from jax.experimental import pallas as pl
from jax.experimental.pallas import tpu as pltpu
from jax.sharding import PartitionSpec as P

HEAD_DIM = 64
STEPS = 2
EPSILON = 1e-05
GELU_COEF = 0.044715
ROOT_TWO_PI = math.sqrt(2.0 / math.pi)
LANES = 128
BF16 = jnp.bfloat16
F32 = jnp.float32


def norm_pair(values, tangent, norm_gain):
    meansq = jnp.mean(values * values, axis=-1, keepdims=True) + EPSILON
    inverse = lax.rsqrt(meansq)
    inner_mean = jnp.mean(values * tangent, axis=-1, keepdims=True)
    primal = values * inverse * norm_gain
    derived = (tangent * inverse - values * (inverse * inverse * inverse * inner_mean)) * norm_gain
    return (primal.astype(BF16), derived.astype(BF16))


def gelu_pair(pre_act, tangent):
    square = pre_act * pre_act
    tanh_value = jnp.tanh(ROOT_TWO_PI * pre_act * (1.0 + GELU_COEF * square))
    half = 0.5 * (1.0 + tanh_value)
    slope_value = half + 0.5 * pre_act * (1.0 - tanh_value * tanh_value) * (
        ROOT_TWO_PI * (1.0 + 3.0 * GELU_COEF * square)
    )
    return ((pre_act * half).astype(BF16), (slope_value * tangent).astype(BF16))


def dot(a, b):
    return jnp.dot(a, b, preferred_element_type=F32)


def dot_t(a, b):
    return lax.dot_general(a, b, (((1,), (1,)), ((), ())), preferred_element_type=F32)


def flow_kernel(
    n,
    m,
    latent,
    probe,
    time_embed,
    gain_attn,
    gain_mlp,
    w_query,
    w_key,
    w_value,
    w_out,
    w_in,
    w_down,
    latent_end,
    stats_out,
    mean_out,
    wqkv,
    wout,
    win,
    wdown,
    normed,
    qbuf,
    kbuf,
    vbuf,
    headbuf,
    headsend,
    headall,
    midbuf,
    partial,
    rssend,
    rsrecv,
    state,
    statbuf,
    sumbuf,
    wsem,
    wsend,
    wrecv,
    kvsend,
    kvrecv,
    zsend,
    zrecv,
    ssend,
    srecv,
    msend,
    mrecv,
):
    s = lax.axis_index("seq")
    z = lax.axis_index("head")
    rows, width = latent.shape
    part = rows // m
    cols = w_query.shape[1]
    pairs = cols // LANES

    def flip(bit):
        return s + bit - 2 * bit * lax.rem(s // bit, 2)

    def zpeer(d):
        return lax.rem(z + d, m)

    def zfrom(d):
        return lax.rem(z + m - d, m)

    def remote(src, dst, send, recv, target_s, target_z):
        return pltpu.make_async_remote_copy(
            src_ref=src,
            dst_ref=dst,
            send_sem=send,
            recv_sem=recv,
            device_id=(target_s, target_z),
            device_id_type=pl.DeviceIdType.MESH,
        )

    loads = [
        pltpu.make_async_copy(w_query, wqkv.at[:, pl.ds(0, cols)], wsem.at[0]),
        pltpu.make_async_copy(w_key, wqkv.at[:, pl.ds(cols, cols)], wsem.at[1]),
        pltpu.make_async_copy(w_value, wqkv.at[:, pl.ds(2 * cols, cols)], wsem.at[2]),
        pltpu.make_async_copy(w_out, wout.at[z], wsem.at[3]),
        pltpu.make_async_copy(w_in, win, wsem.at[4]),
        pltpu.make_async_copy(w_down, wdown, wsem.at[5]),
    ]
    for load in loads:
        load.start()

    barrier = pltpu.get_barrier_semaphore()
    for d in range(1, m):
        pl.semaphore_signal(
            barrier, inc=1, device_id=(s, zpeer(d)), device_id_type=pl.DeviceIdType.MESH
        )
    for d in range(1, n):
        pl.semaphore_signal(
            barrier,
            inc=1,
            device_id=(lax.rem(s + d, n), z),
            device_id_type=pl.DeviceIdType.MESH,
        )

    def put_pair(ref, j, pair):
        ref[j, :part, :] = pair[0]
        ref[j, part:, :] = pair[1]

    for j in range(m):
        span = slice(j * part, (j + 1) * part)
        put_pair(
            normed.at[0],
            j,
            norm_pair(latent[span, :].astype(F32), probe[span, :].astype(F32), gain_attn[...]),
        )
    own = pl.ds(pl.multiple_of(z * part, part), part)
    direction = probe[own, :].astype(F32)
    state[...] = latent[own, :].astype(F32)

    pl.semaphore_wait(barrier, n + m - 2)

    half = cols // 2
    core = lax.rem(s, 2)
    mine = pl.ds(pl.multiple_of(core * half, half), half)
    other = pl.ds(pl.multiple_of((1 - core) * half, half), half)
    partner = flip(1)
    loads[3].wait()
    w_copies = []
    for d in range(1, m):
        copy = remote(
            wout.at[z, mine], wout.at[z, mine], wsend.at[0, d], wrecv.at[0, d], s, zpeer(d)
        )
        copy.start()
        w_copies.append(copy)

    def kv_exchange(k):
        bufs = (kbuf, vbuf)
        sends = []

        def give(which, rel, slot, target, at):
            copy = remote(
                bufs[which].at[k, slot],
                bufs[which].at[k, slot],
                kvsend.at[k, which, len(sends)],
                kvrecv.at[k, which, at],
                target,
                z,
            )
            copy.start()
            sends.append(copy)

        def got(which, slot, at):
            pltpu.make_async_copy(
                bufs[which].at[k, slot], bufs[which].at[k, slot], kvrecv.at[k, which, at]
            ).wait()

        if n == 8:
            xn, yn, dn = flip(2), flip(4), lax.rem(s + 4, 8)
            dn = dn + 2 - 4 * lax.rem(dn // 2, 2)
            give(0, 0, s, xn, 2)
            give(1, 0, s, yn, 4)
            give(0, 0, s, yn, 4)
            give(1, 0, s, xn, 2)
            give(0, 0, s, partner, 1)
            give(1, 0, s, partner, 1)
            got(0, xn, 2)
            give(0, 2, xn, yn, 6)
            give(0, 2, xn, partner, 3)
            got(1, yn, 4)
            give(1, 4, yn, xn, 6)
            give(1, 4, yn, partner, 5)
            got(0, yn, 4)
            give(0, 4, yn, partner, 5)
            got(1, xn, 2)
            give(1, 2, xn, partner, 3)
            got(0, dn, 6)
            give(0, 6, dn, partner, 7)
            got(1, dn, 6)
            give(1, 6, dn, partner, 7)

            def across(base):
                return base + 1 - 2 * lax.rem(base, 2)

            keys_left = [(0, across(t), r) for t, r in ((s, 1), (xn, 3), (yn, 5), (dn, 7))]
            vals_left = [(1, across(t), r) for t, r in ((s, 1), (xn, 3), (yn, 5), (dn, 7))]
        else:
            for d in range(1, n):
                for which in range(2):
                    give(which, d, s, lax.rem(s + d, n), d)
            keys_left = [(0, lax.rem(s + n - d, n), d) for d in range(1, n)]
            vals_left = [(1, lax.rem(s + n - d, n), d) for d in range(1, n)]
        return sends, keys_left, vals_left, got

    lane = lax.broadcasted_iota(jnp.int32, (1, LANES), 1)
    scale = HEAD_DIM ** (-0.5)
    frames = rows * n

    for k in range(STEPS):
        if k == 0:
            for load in loads[:3]:
                load.wait()
        stacked = normed[k].reshape(2 * rows, width)

        def project(which):
            both = dot(stacked, wqkv[:, which * cols : (which + 1) * cols]).astype(BF16)
            both = both.reshape(m, 2, part, cols)
            return both[:, 0].reshape(rows, cols), both[:, 1].reshape(rows, cols)

        for which, ref in ((1, kbuf), (2, vbuf)):
            prim, tang = project(which)
            ref[k, s, 0] = prim
            ref[k, s, 1] = tang
        sends, keys_left, vals_left, got = kv_exchange(k)
        prim, tang = project(0)
        qbuf[0] = prim
        qbuf[1] = tang
        for item in keys_left + vals_left:
            got(*item)

        @pl.loop(0, pairs)
        def _(p):
            at = pl.ds(pl.multiple_of(p * LANES, LANES), LANES)
            keys = kbuf[k, :, 0, :, at].reshape(frames, LANES)
            key_tang = kbuf[k, :, 1, :, at].reshape(frames, LANES)
            vals = vbuf[k, :, 0, :, at].reshape(frames, LANES)
            val_tang = vbuf[k, :, 1, :, at].reshape(frames, LANES)
            both_keys = jnp.concatenate([keys, key_tang], axis=1)
            both_vals = jnp.concatenate([vals, val_tang], axis=1)
            queries = qbuf[0, :, at]
            query_tang = qbuf[1, :, at]
            zero = jnp.zeros_like(queries)
            prims, tangs = [], []
            for side in range(LANES // HEAD_DIM):
                keep = (lane // HEAD_DIM) == side
                q = jnp.where(keep, queries, zero)
                qt = jnp.where(keep, query_tang, zero)
                left = jnp.concatenate(
                    [jnp.concatenate([q, zero], axis=1), jnp.concatenate([qt, q], axis=1)], axis=0
                )
                both = dot_t(left, both_keys) * scale
                scores, score_tang = both[:rows], both[rows:]
                weights = jnp.exp(scores - jnp.max(scores, axis=-1, keepdims=True))
                weighted = weights * score_tang
                total = jnp.sum(weights, axis=-1, keepdims=True)
                carried = jnp.sum(weighted, axis=-1, keepdims=True)
                rounded = jnp.concatenate([weights.astype(BF16), weighted.astype(BF16)], axis=0)
                mixed = dot(rounded, both_vals)
                prim = mixed[:rows, :LANES] / total
                tang = (mixed[rows:, :LANES] + mixed[:rows, LANES:]) / total - (
                    carried / total
                ) * prim
                prims.append(prim)
                tangs.append(tang)
            first = (lane // HEAD_DIM) == 0
            headbuf[0, :, at] = jnp.where(first, prims[0], prims[1]).astype(BF16)
            headbuf[1, :, at] = jnp.where(first, tangs[0], tangs[1]).astype(BF16)

        for j in range(m):
            headsend[k, j, :part, :] = headbuf[0, j * part : (j + 1) * part, :]
            headsend[k, j, part:, :] = headbuf[1, j * part : (j + 1) * part, :]

        def z_start(phase, src_of, dst):
            copies = []
            for d in range(m - 1, 0, -1):
                copy = remote(
                    src_of(zpeer(d)),
                    dst,
                    zsend.at[k, phase, d],
                    zrecv.at[k, phase, d],
                    s,
                    zpeer(d),
                )
                copy.start()
                copies.append(copy)
            return copies

        def z_wait(copies):
            for copy in copies:
                copy.wait_send()
                copy.wait_recv()

        copies = z_start(0, lambda j: headsend.at[k, j], headall.at[k, z])
        headall[k, z] = headsend[k, z]
        if k == 0:
            forwards = []
            for d, copy in zip(range(1, m), w_copies):
                copy.wait_send()
                copy.wait_recv()
                forward = remote(
                    wout.at[zfrom(d), mine],
                    wout.at[zfrom(d), mine],
                    wsend.at[1, d],
                    wrecv.at[1, d],
                    partner,
                    z,
                )
                forward.start()
                forwards.append(forward)
            for forward in forwards:
                forward.wait_send()
                forward.wait_recv()
        z_wait(copies)
        attn_both = jnp.zeros((2 * part, width), F32)
        for j in range(m):
            attn_both = attn_both + dot(headall[k, j], wout[j])
        inputs = state[...]
        if k > 0:
            inputs = inputs + (k / STEPS) * time_embed[...]
        put_pair(
            midbuf.at[k],
            z,
            norm_pair(inputs + attn_both[:part], direction + attn_both[part:], gain_mlp[...]),
        )
        copies = z_start(1, lambda j: midbuf.at[k, z], midbuf.at[k, z])
        if k == 0:
            loads[4].wait()
            loads[5].wait()
        z_wait(copies)
        pre = dot(midbuf[k].reshape(2 * rows, width), win[...]).reshape(m, 2, part, win.shape[1])
        act, act_tang = gelu_pair(pre[:, 0], pre[:, 1])
        acts = jnp.concatenate([act, act_tang], axis=1).reshape(2 * rows, win.shape[1])
        partial[...] = dot(acts, wdown[...]).reshape(m, 2 * part, width)
        rssend[k] = partial[...].astype(BF16)
        copies = z_start(2, lambda j: rssend.at[k, j], rsrecv.at[k, z])
        z_wait(copies)
        both = attn_both + partial[z]
        for d in range(1, m):
            both = both + rsrecv[k, zfrom(d)].astype(F32)
        trace_add = jnp.sum(direction * both[part:], axis=-1, keepdims=True) / (STEPS * width)
        trace = trace_add if k == 0 else trace + trace_add
        new_state = state[...] + both[:part] / STEPS
        state[...] = new_state
        last = k == STEPS - 1
        if not last:
            following = new_state + ((k + 1) / STEPS) * time_embed[...]
            put_pair(normed.at[k + 1], z, norm_pair(following, direction, gain_attn[...]))
        else:
            logp = (
                trace
                - 0.5 * jnp.sum(new_state * new_state, axis=-1, keepdims=True) / width
                - 0.5 * math.log(2.0 * math.pi)
            )
            statbuf[z] = jnp.where(lane == 0, trace, logp)
            stat_copies = []
            for d in range(1, m):
                copy = remote(
                    statbuf.at[z], statbuf.at[z], ssend.at[d], srecv.at[d], s, zpeer(d)
                )
                copy.start()
                stat_copies.append(copy)
            high = new_state.astype(BF16)
            put_pair(normed.at[k + 1], z, (high, (new_state - high.astype(F32)).astype(BF16)))
        copies = z_start(3, lambda j: normed.at[k + 1, z], normed.at[k + 1, z])
        for send in sends:
            send.wait_send()
        if last:
            z_wait(stat_copies)
            stats = statbuf[...].reshape(rows, LANES)
            sumbuf[s] = jnp.broadcast_to(
                jnp.sum(stats.reshape(rows // 8, 8, LANES), axis=0), (8, LANES)
            )
            mean_copies = []
            for d in range(1, n):
                copy = remote(
                    sumbuf.at[s], sumbuf.at[s], msend.at[d], mrecv.at[d], lax.rem(s + d, n), z
                )
                copy.start()
                mean_copies.append(copy)
            stats_out[...] = jnp.transpose(stats)[:8, :]
        z_wait(copies)
    final = normed[STEPS].reshape(m, 2, part, width).astype(F32)
    latent_end[...] = (final[:, 0] + final[:, 1]).reshape(rows, width)
    z_wait(mean_copies)
    sums = jnp.sum(sumbuf[...], axis=0)
    mean_out[...] = jnp.broadcast_to(jnp.sum(sums, axis=0, keepdims=True) / frames, (8, LANES))


def per_device(
    n,
    m,
    latent,
    probe,
    time_embed,
    gain_attn,
    w_query,
    w_key,
    w_value,
    w_out,
    gain_mlp,
    w_in,
    w_down,
):
    rows, width = latent.shape
    cols = w_query.shape[1]
    hidden = w_in.shape[1]
    part = rows // m
    vmem = pl.BlockSpec(memory_space=pltpu.VMEM)
    anyspace = pl.BlockSpec(memory_space=pl.ANY)
    dma = pltpu.SemaphoreType.DMA
    state, stats, mean = pl.pallas_call(
        functools.partial(flow_kernel, n, m),
        out_shape=(
            jax.ShapeDtypeStruct((rows, width), F32),
            jax.ShapeDtypeStruct((8, rows), F32),
            jax.ShapeDtypeStruct((8, LANES), F32),
        ),
        in_specs=[vmem] * 5 + [anyspace] * 6,
        out_specs=(vmem, vmem, vmem),
        scratch_shapes=[
            pltpu.VMEM((width, 3 * cols), BF16),
            pltpu.VMEM((m, cols, width), BF16),
            pltpu.VMEM((width, hidden), BF16),
            pltpu.VMEM((hidden, width), BF16),
            pltpu.VMEM((STEPS + 1, m, 2 * part, width), BF16),
            pltpu.VMEM((2, rows, cols), BF16),
            pltpu.VMEM((STEPS, n, 2, rows, cols), BF16),
            pltpu.VMEM((STEPS, n, 2, rows, cols), BF16),
            pltpu.VMEM((2, rows, cols), BF16),
            pltpu.VMEM((STEPS, m, 2 * part, cols), BF16),
            pltpu.VMEM((STEPS, m, 2 * part, cols), BF16),
            pltpu.VMEM((STEPS, m, 2 * part, width), BF16),
            pltpu.VMEM((m, 2 * part, width), F32),
            pltpu.VMEM((STEPS, m, 2 * part, width), BF16),
            pltpu.VMEM((STEPS, m, 2 * part, width), BF16),
            pltpu.VMEM((part, width), F32),
            pltpu.VMEM((m, part, LANES), F32),
            pltpu.VMEM((n, 8, LANES), F32),
            dma((6,)),
            dma((2, m)),
            dma((2, m)),
            dma((STEPS, 2, 2 * n)),
            dma((STEPS, 2, n)),
            dma((STEPS, 4, m)),
            dma((STEPS, 4, m)),
            dma((m,)),
            dma((m,)),
            dma((n,)),
            dma((n,)),
        ],
        compiler_params=pltpu.CompilerParams(
            collective_id=0, has_side_effects=True, vmem_limit_bytes=60 * 1024 * 1024
        ),
    )(
        latent,
        probe,
        time_embed.reshape(1, width),
        gain_attn.reshape(1, width),
        gain_mlp.reshape(1, width),
        w_query,
        w_key,
        w_value,
        w_out,
        w_in,
        w_down,
    )
    return (state, stats[0], stats[1], mean[0, 1])


def solution(mesh):
    return jax.shard_map(
        functools.partial(per_device, mesh.shape["seq"], mesh.shape["head"]),
        mesh=mesh,
        in_specs=(
            P("seq", None),
            P("seq", None),
            P(),
            P(),
            P(None, "head"),
            P(None, "head"),
            P(None, "head"),
            P("head", None),
            P(),
            P(None, "head"),
            P("head", None),
        ),
        out_specs=(P("seq", None), P("seq"), P("seq"), P()),
        check_vma=False,
    )
```

```python
import functools
import math

import jax
import jax.numpy as jnp
from jax import lax
from jax.experimental import pallas as pl
from jax.experimental.pallas import tpu as pltpu
from jax.sharding import PartitionSpec as P

HEAD_DIM = 64
STEPS = 2
EPSILON = 1e-05
GELU_COEF = 0.044715
ROOT_TWO_PI = math.sqrt(2.0 / math.pi)
LANES = 128
HALVES = 2
BF16 = jnp.bfloat16
F32 = jnp.float32


def norm_pair(values, tangent, norm_gain):
    meansq = jnp.mean(values * values, axis=-1, keepdims=True) + EPSILON
    inverse = lax.rsqrt(meansq)
    inner_mean = jnp.mean(values * tangent, axis=-1, keepdims=True)
    primal = values * inverse * norm_gain
    derived = (tangent * inverse - values * (inverse * inverse * inverse * inner_mean)) * norm_gain
    return (primal.astype(BF16), derived.astype(BF16))


def gelu_pair(pre_act, tangent):
    square = pre_act * pre_act
    tanh_value = jnp.tanh(ROOT_TWO_PI * pre_act * (1.0 + GELU_COEF * square))
    half = 0.5 * (1.0 + tanh_value)
    slope_value = half + 0.5 * pre_act * (1.0 - tanh_value * tanh_value) * (
        ROOT_TWO_PI * (1.0 + 3.0 * GELU_COEF * square)
    )
    return ((pre_act * half).astype(BF16), (slope_value * tangent).astype(BF16))


def dot(a, b):
    return jnp.dot(a, b, preferred_element_type=F32)


def dot_t(a, b):
    return lax.dot_general(a, b, (((1,), (1,)), ((), ())), preferred_element_type=F32)


def flow_kernel(
    n,
    m,
    latent,
    probe,
    time_embed,
    gain_attn,
    gain_mlp,
    w_query,
    w_key,
    w_value,
    w_out,
    w_in,
    w_down,
    latent_end,
    stats_out,
    mean_out,
    wqkv,
    wout,
    win,
    wdown,
    normed,
    qbuf,
    kbuf,
    vbuf,
    headall,
    inbuf,
    probe_down,
    partial,
    rssend,
    rsrecv,
    state,
    delta,
    tracebuf,
    tilebuf,
    sumbuf,
    wsem,
    wsend,
    wrecv,
    kvsend,
    kvrecv,
    zsend,
    zrecv,
    ssend,
    srecv,
    msend,
    mrecv,
):
    s = lax.axis_index("seq")
    z = lax.axis_index("head")
    rows, width = latent.shape
    hrows = rows // HALVES
    part = hrows // m
    cols = w_query.shape[1]
    pairs = cols // LANES

    def flip(bit):
        return s + bit - 2 * bit * lax.rem(s // bit, 2)

    def zpeer(d):
        return lax.rem(z + d, m)

    def zfrom(d):
        return lax.rem(z + m - d, m)

    def remote(src, dst, send, recv, target_s, target_z):
        return pltpu.make_async_remote_copy(
            src_ref=src,
            dst_ref=dst,
            send_sem=send,
            recv_sem=recv,
            device_id=(target_s, target_z),
            device_id_type=pl.DeviceIdType.MESH,
        )

    loads = [
        pltpu.make_async_copy(w_query, wqkv.at[:, pl.ds(0, cols)], wsem.at[0]),
        pltpu.make_async_copy(w_key, wqkv.at[:, pl.ds(cols, cols)], wsem.at[1]),
        pltpu.make_async_copy(w_value, wqkv.at[:, pl.ds(2 * cols, cols)], wsem.at[2]),
        pltpu.make_async_copy(w_out, wout.at[z], wsem.at[3]),
        pltpu.make_async_copy(w_in, win, wsem.at[4]),
        pltpu.make_async_copy(w_down, wdown, wsem.at[5]),
    ]
    for load in loads:
        load.start()

    barrier = pltpu.get_barrier_semaphore()
    for d in range(1, m):
        pl.semaphore_signal(
            barrier, inc=1, device_id=(s, zpeer(d)), device_id_type=pl.DeviceIdType.MESH
        )
    for d in range(1, n):
        pl.semaphore_signal(
            barrier,
            inc=1,
            device_id=(lax.rem(s + d, n), z),
            device_id_type=pl.DeviceIdType.MESH,
        )

    def own_rows(h):
        return pl.ds(pl.multiple_of(h * hrows + z * part, part), part)

    def norm_all():
        for h in range(HALVES):
            span = slice(h * hrows, (h + 1) * hrows)
            prim, tang = norm_pair(inbuf[span, :], probe[span, :].astype(F32), gain_attn[...])
            normed[span, :] = prim
            normed[rows + h * hrows : rows + (h + 1) * hrows, :] = tang

    inbuf[...] = latent[...].astype(F32)
    norm_all()
    for h in range(HALVES):
        state[h] = latent[own_rows(h), :].astype(F32)

    pl.semaphore_wait(barrier, n + m - 2)

    half = cols // 2
    core = lax.rem(s, 2)
    mine = pl.ds(pl.multiple_of(core * half, half), half)
    other = pl.ds(pl.multiple_of((1 - core) * half, half), half)
    partner = flip(1)
    loads[3].wait()
    w_copies = []
    for d in range(1, m):
        copy = remote(
            wout.at[z, mine], wout.at[z, mine], wsend.at[0, d], wrecv.at[0, d], s, zpeer(d)
        )
        copy.start()
        w_copies.append(copy)

    def kv_exchange(k):
        bufs = (kbuf, vbuf)
        sends = []

        def give(which, rel, slot, target, at):
            copy = remote(
                bufs[which].at[k, slot],
                bufs[which].at[k, slot],
                kvsend.at[k, which, len(sends)],
                kvrecv.at[k, which, at],
                target,
                z,
            )
            copy.start()
            sends.append(copy)

        def got(which, slot, at):
            pltpu.make_async_copy(
                bufs[which].at[k, slot], bufs[which].at[k, slot], kvrecv.at[k, which, at]
            ).wait()

        xn, yn = flip(2), flip(4)
        dn = yn + 2 - 4 * lax.rem(yn // 2, 2)

        def own(which):
            if n == 8:
                first, second = ((xn, 2), (yn, 4)) if which == 0 else ((yn, 4), (xn, 2))
                give(which, 0, s, *first)
                give(which, 0, s, *second)
                give(which, 0, s, partner, 1)
            else:
                for d in range(1, n):
                    give(which, d, s, lax.rem(s + d, n), d)

        def rest():
            if n != 8:
                return [[(w, lax.rem(s + n - d, n), d) for d in range(1, n)] for w in range(2)]
            got(0, xn, 2)
            give(0, 2, xn, yn, 6)
            give(0, 2, xn, partner, 3)
            got(1, yn, 4)
            give(1, 4, yn, xn, 6)
            give(1, 4, yn, partner, 5)
            got(0, yn, 4)
            give(0, 4, yn, partner, 5)
            got(1, xn, 2)
            give(1, 2, xn, partner, 3)
            got(0, dn, 6)
            give(0, 6, dn, partner, 7)
            got(1, dn, 6)
            give(1, 6, dn, partner, 7)

            def across(base):
                return base + 1 - 2 * lax.rem(base, 2)

            slots = ((s, 1), (xn, 3), (yn, 5), (dn, 7))
            return [[(w, across(t), r) for t, r in slots] for w in range(2)]

        return sends, own, rest, got

    lane = lax.broadcasted_iota(jnp.int32, (1, LANES), 1)
    scale = HEAD_DIM ** (-0.5)
    frames = rows * n
    trace = [None] * HALVES

    for k in range(STEPS):

        def project(which):
            if k == 0:
                loads[which].wait()
            weight = wqkv[:, which * cols : (which + 1) * cols]
            return dot(normed[...], weight).astype(BF16).reshape(2, rows, cols)

        def z_start(phase, src_of, dst):
            copies = []
            for d in range(m - 1, 0, -1):
                copy = remote(
                    src_of(zpeer(d)),
                    dst,
                    zsend.at[k, phase, d],
                    zrecv.at[k, phase, d],
                    s,
                    zpeer(d),
                )
                copy.start()
                copies.append(copy)
            return copies

        def z_wait(copies):
            for copy in copies:
                copy.wait_send()
                copy.wait_recv()

        sends, own, rest, got = kv_exchange(k)
        kbuf[k, s] = project(1)
        own(0)
        vbuf[k, s] = project(2)
        own(1)
        qbuf[...] = project(0)
        if k == 0:
            loads[5].wait()
            probe_down[...] = dot_t(probe[...], wdown[...])
        for group in rest():
            for item in group:
                got(*item)

        head_copies = []
        for h in range(HALVES):
            span = slice(h * hrows, (h + 1) * hrows)

            @pl.loop(0, pairs)
            def _(p):
                at = pl.ds(pl.multiple_of(p * LANES, LANES), LANES)
                keys = kbuf[k, :, 0, :, at].reshape(frames, LANES)
                key_tang = kbuf[k, :, 1, :, at].reshape(frames, LANES)
                vals = vbuf[k, :, 0, :, at].reshape(frames, LANES)
                val_tang = vbuf[k, :, 1, :, at].reshape(frames, LANES)
                both_keys = jnp.concatenate([keys, key_tang], axis=1)
                both_vals = jnp.concatenate([vals, val_tang], axis=1)
                queries = qbuf[0, span, at]
                query_tang = qbuf[1, span, at]
                zero = jnp.zeros_like(queries)
                left = []
                for side in range(LANES // HEAD_DIM):
                    keep = (lane // HEAD_DIM) == side
                    q = jnp.where(keep, queries, zero)
                    qt = jnp.where(keep, query_tang, zero)
                    left.append(
                        (
                            jnp.concatenate([q, zero], axis=1),
                            jnp.concatenate([qt, q], axis=1),
                        )
                    )
                stack = [item[0] for item in left] + [item[1] for item in left]
                both = dot_t(jnp.concatenate(stack, axis=0), both_keys) * scale
                scores, score_tang = both[: 2 * hrows], both[2 * hrows :]
                weights = jnp.exp(scores - jnp.max(scores, axis=-1, keepdims=True))
                weighted = weights * score_tang
                total = jnp.sum(weights, axis=-1, keepdims=True)
                carried = jnp.sum(weighted, axis=-1, keepdims=True)
                rounded = jnp.concatenate([weights.astype(BF16), weighted.astype(BF16)], axis=0)
                mixed = dot(rounded, both_vals)
                prim = mixed[: 2 * hrows, :LANES] / total
                tang = (mixed[2 * hrows :, :LANES] + mixed[: 2 * hrows, LANES:]) / total - (
                    carried / total
                ) * prim
                first = (lane // HEAD_DIM) == 0
                headall[k, h, z, 0, :, at] = jnp.where(first, prim[:hrows], prim[hrows:]).astype(
                    BF16
                )
                headall[k, h, z, 1, :, at] = jnp.where(first, tang[:hrows], tang[hrows:]).astype(
                    BF16
                )

            head_copies.append(z_start(h, lambda j: headall.at[k, h, z], headall.at[k, h, z]))

        if k == 0:
            forwards = []
            for d, copy in zip(range(1, m), w_copies):
                copy.wait_send()
                copy.wait_recv()
                forward = remote(
                    wout.at[zfrom(d), mine],
                    wout.at[zfrom(d), mine],
                    wsend.at[1, d],
                    wrecv.at[1, d],
                    partner,
                    z,
                )
                forward.start()
                forwards.append(forward)
            loads[4].wait()
            for forward in forwards:
                forward.wait_send()
                forward.wait_recv()

        rs_copies = []
        for h in range(HALVES):
            span = slice(h * hrows, (h + 1) * hrows)
            z_wait(head_copies[h])
            attn_both = jnp.zeros((2 * hrows, width), F32)
            for j in range(m):
                attn_both = attn_both + dot(
                    headall[k, h, j].reshape(2 * hrows, cols), wout[j]
                )
            attn, attn_tang = attn_both[:hrows], attn_both[hrows:]
            direction = probe[span, :].astype(F32)
            pair = norm_pair(inbuf[span, :] + attn, direction + attn_tang, gain_mlp[...])
            pre = dot(jnp.concatenate(pair, axis=0), win[...])
            act, act_tang = gelu_pair(pre[:hrows], pre[hrows:])
            terms = dot(act, wdown[...])
            rssend[k, h] = terms.astype(BF16).reshape(m, part, width)
            rs_copies.append(
                z_start(HALVES + h, lambda j: rssend.at[k, h, j], rsrecv.at[k, h, z])
            )
            partial[h] = (attn + terms).reshape(m, part, width)
            grown = jnp.sum(direction * attn_tang, axis=-1, keepdims=True) / m + jnp.sum(
                act_tang.astype(F32) * probe_down[span, :], axis=-1, keepdims=True
            )
            trace[h] = grown if k == 0 else trace[h] + grown

        last = k == STEPS - 1
        if last:
            column = jnp.concatenate(trace, axis=0) / (STEPS * width)
            trace_sum = jnp.sum(column, axis=0, keepdims=True)
            tracebuf[z] = jnp.transpose(jnp.broadcast_to(column, (rows, LANES)))[:8, :]
            trace_copies = []
            for d in range(1, m):
                copy = remote(
                    tracebuf.at[z], tracebuf.at[z], ssend.at[0, d], srecv.at[0, d], s, zpeer(d)
                )
                copy.start()
                trace_copies.append(copy)

        delta_copies = []
        squares = jnp.zeros((1, 1), F32)
        for h in range(HALVES):
            z_wait(rs_copies[h])
            field = partial[h, z]
            for d in range(1, m):
                field = field + rsrecv[k, h, zfrom(d)].astype(F32)
            new_state = state[h] + field / STEPS
            state[h] = new_state
            delta[k, h, z] = (new_state - latent[own_rows(h), :].astype(F32)).astype(BF16)
            delta_copies.append(
                z_start(2 * HALVES + h, lambda j: delta.at[k, h, z], delta.at[k, h, z])
            )
            if last:
                by_row = jnp.sum(new_state * new_state, axis=-1, keepdims=True)
                squares = squares + jnp.sum(by_row, axis=0, keepdims=True)
        for send in sends:
            send.wait_send()
        if last:
            share = trace_sum - 0.5 * squares / width
            tilebuf[z] = jnp.broadcast_to(share, (8, LANES))
            tile_copies = []
            for d in range(1, m):
                copy = remote(
                    tilebuf.at[z], tilebuf.at[z], ssend.at[1, d], srecv.at[1, d], s, zpeer(d)
                )
                copy.start()
                tile_copies.append(copy)
            z_wait(trace_copies)
            trace_row = jnp.sum(tracebuf[...], axis=0)
            z_wait(tile_copies)
            sumbuf[s] = jnp.sum(tilebuf[...], axis=0)
            mean_copies = []
            for d in range(1, n):
                copy = remote(
                    sumbuf.at[s], sumbuf.at[s], msend.at[d], mrecv.at[d], lax.rem(s + d, n), z
                )
                copy.start()
                mean_copies.append(copy)
        norms = []
        for h in range(HALVES):
            span = slice(h * hrows, (h + 1) * hrows)
            z_wait(delta_copies[h])
            following = latent[span, :].astype(F32) + delta[k, h].reshape(hrows, width).astype(F32)
            if last:
                latent_end[span, :] = following
                norms.append(jnp.sum(following * following, axis=-1, keepdims=True))
            else:
                following = following + ((k + 1) / STEPS) * time_embed[...]
                inbuf[span, :] = following
                prim, tang = norm_pair(following, probe[span, :].astype(F32), gain_attn[...])
                normed[span, :] = prim
                normed[rows + h * hrows : rows + (h + 1) * hrows, :] = tang
    norm_row = jnp.transpose(jnp.broadcast_to(jnp.concatenate(norms, axis=0), (rows, LANES)))[:8]
    half_log = 0.5 * math.log(2.0 * math.pi)
    first_row = lax.broadcasted_iota(jnp.int32, (8, rows), 0) == 0
    stats_out[...] = jnp.where(
        first_row, trace_row, trace_row - 0.5 * norm_row / width - half_log
    )
    z_wait(mean_copies)
    mean_out[...] = jnp.sum(sumbuf[...], axis=0) / frames - half_log


def per_device(
    n,
    m,
    latent,
    probe,
    time_embed,
    gain_attn,
    w_query,
    w_key,
    w_value,
    w_out,
    gain_mlp,
    w_in,
    w_down,
):
    rows, width = latent.shape
    cols = w_query.shape[1]
    hidden = w_in.shape[1]
    hrows = rows // HALVES
    part = hrows // m
    vmem = pl.BlockSpec(memory_space=pltpu.VMEM)
    anyspace = pl.BlockSpec(memory_space=pl.ANY)
    dma = pltpu.SemaphoreType.DMA
    state, stats, mean = pl.pallas_call(
        functools.partial(flow_kernel, n, m),
        out_shape=(
            jax.ShapeDtypeStruct((rows, width), F32),
            jax.ShapeDtypeStruct((8, rows), F32),
            jax.ShapeDtypeStruct((8, LANES), F32),
        ),
        in_specs=[vmem] * 5 + [anyspace] * 6,
        out_specs=(vmem, vmem, vmem),
        scratch_shapes=[
            pltpu.VMEM((width, 3 * cols), BF16),
            pltpu.VMEM((m, cols, width), BF16),
            pltpu.VMEM((width, hidden), BF16),
            pltpu.VMEM((hidden, width), BF16),
            pltpu.VMEM((2 * rows, width), BF16),
            pltpu.VMEM((2, rows, cols), BF16),
            pltpu.VMEM((STEPS, n, 2, rows, cols), BF16),
            pltpu.VMEM((STEPS, n, 2, rows, cols), BF16),
            pltpu.VMEM((STEPS, HALVES, m, 2, hrows, cols), BF16),
            pltpu.VMEM((rows, width), F32),
            pltpu.VMEM((rows, hidden), F32),
            pltpu.VMEM((HALVES, m, part, width), F32),
            pltpu.VMEM((STEPS, HALVES, m, part, width), BF16),
            pltpu.VMEM((STEPS, HALVES, m, part, width), BF16),
            pltpu.VMEM((HALVES, part, width), F32),
            pltpu.VMEM((STEPS, HALVES, m, part, width), BF16),
            pltpu.VMEM((m, 8, rows), F32),
            pltpu.VMEM((m, 8, LANES), F32),
            pltpu.VMEM((n, 8, LANES), F32),
            dma((6,)),
            dma((2, m)),
            dma((2, m)),
            dma((STEPS, 2, 2 * n)),
            dma((STEPS, 2, n)),
            dma((STEPS, 3 * HALVES, m)),
            dma((STEPS, 3 * HALVES, m)),
            dma((2, m)),
            dma((2, m)),
            dma((n,)),
            dma((n,)),
        ],
        compiler_params=pltpu.CompilerParams(
            collective_id=0, has_side_effects=True, vmem_limit_bytes=60 * 1024 * 1024
        ),
    )(
        latent,
        probe,
        time_embed.reshape(1, width),
        gain_attn.reshape(1, width),
        gain_mlp.reshape(1, width),
        w_query,
        w_key,
        w_value,
        w_out,
        w_in,
        w_down,
    )
    return (state, stats[0], stats[1], mean[0, 0])


def solution(mesh):
    return jax.shard_map(
        functools.partial(per_device, mesh.shape["seq"], mesh.shape["head"]),
        mesh=mesh,
        in_specs=(
            P("seq", None),
            P("seq", None),
            P(),
            P(),
            P(None, "head"),
            P(None, "head"),
            P(None, "head"),
            P("head", None),
            P(),
            P(None, "head"),
            P("head", None),
        ),
        out_specs=(P("seq", None), P("seq"), P("seq"), P()),
        check_vma=False,
    )
```

```python
import functools
import math

import jax
import jax.numpy as jnp
from jax import lax
from jax.experimental import pallas as pl
from jax.experimental.pallas import tpu as pltpu
from jax.sharding import PartitionSpec as P

HEAD_DIM = 64
STEPS = 2
EPSILON = 1e-05
GELU_COEF = 0.044715
ROOT_TWO_PI = math.sqrt(2.0 / math.pi)
LANES = 128
HALVES = 2
BF16 = jnp.bfloat16
F32 = jnp.float32


def norm_pair(values, tangent, norm_gain):
    meansq = jnp.mean(values * values, axis=-1, keepdims=True) + EPSILON
    inverse = lax.rsqrt(meansq)
    inner_mean = jnp.mean(values * tangent, axis=-1, keepdims=True)
    primal = values * inverse * norm_gain
    derived = (tangent * inverse - values * (inverse * inverse * inverse * inner_mean)) * norm_gain
    return (primal.astype(BF16), derived.astype(BF16))


def gelu_pair(pre_act, tangent):
    square = pre_act * pre_act
    tanh_value = jnp.tanh(ROOT_TWO_PI * pre_act * (1.0 + GELU_COEF * square))
    half = 0.5 * (1.0 + tanh_value)
    slope_value = half + 0.5 * pre_act * (1.0 - tanh_value * tanh_value) * (
        ROOT_TWO_PI * (1.0 + 3.0 * GELU_COEF * square)
    )
    return ((pre_act * half).astype(BF16), (slope_value * tangent).astype(BF16))


def dot(a, b):
    return jnp.dot(a, b, preferred_element_type=F32)


def dot_t(a, b):
    return lax.dot_general(a, b, (((1,), (1,)), ((), ())), preferred_element_type=F32)


def flow_kernel(
    n,
    m,
    latent,
    probe,
    time_embed,
    gain_attn,
    gain_mlp,
    w_query,
    w_key,
    w_value,
    w_out,
    w_in,
    w_down,
    latent_end,
    stats_out,
    mean_out,
    wqkv,
    wout,
    win,
    wdown,
    normed,
    qbuf,
    kbuf,
    vbuf,
    headall,
    inbuf,
    probe_down,
    partial,
    rssend,
    rsrecv,
    state,
    delta,
    tracebuf,
    tilebuf,
    sumbuf,
    wsem,
    wsend,
    wrecv,
    kvsend,
    kvrecv,
    zsend,
    zrecv,
    ssend,
    srecv,
    msend,
    mrecv,
):
    s = lax.axis_index("seq")
    z = lax.axis_index("head")
    rows, width = latent.shape
    hrows = rows // HALVES
    part = hrows // m
    cols = w_query.shape[1]
    pairs = cols // LANES

    def flip(bit):
        return s + bit - 2 * bit * lax.rem(s // bit, 2)

    def zpeer(d):
        return lax.rem(z + d, m)

    def zfrom(d):
        return lax.rem(z + m - d, m)

    def remote(src, dst, send, recv, target_s, target_z):
        return pltpu.make_async_remote_copy(
            src_ref=src,
            dst_ref=dst,
            send_sem=send,
            recv_sem=recv,
            device_id=(target_s, target_z),
            device_id_type=pl.DeviceIdType.MESH,
        )

    loads = [
        pltpu.make_async_copy(w_query, wqkv.at[:, pl.ds(0, cols)], wsem.at[0]),
        pltpu.make_async_copy(w_key, wqkv.at[:, pl.ds(cols, cols)], wsem.at[1]),
        pltpu.make_async_copy(w_value, wqkv.at[:, pl.ds(2 * cols, cols)], wsem.at[2]),
        pltpu.make_async_copy(w_out, wout.at[z], wsem.at[3]),
        pltpu.make_async_copy(w_in, win, wsem.at[4]),
        pltpu.make_async_copy(w_down, wdown, wsem.at[5]),
    ]
    for index in (1, 2, 3, 0, 5, 4):
        loads[index].start()

    barrier = pltpu.get_barrier_semaphore()
    for d in range(1, m):
        pl.semaphore_signal(
            barrier, inc=1, device_id=(s, zpeer(d)), device_id_type=pl.DeviceIdType.MESH
        )
    for d in range(1, n):
        pl.semaphore_signal(
            barrier,
            inc=1,
            device_id=(lax.rem(s + d, n), z),
            device_id_type=pl.DeviceIdType.MESH,
        )

    def own_rows(h):
        return pl.ds(pl.multiple_of(h * hrows + z * part, part), part)

    def norm_all():
        for h in range(HALVES):
            span = slice(h * hrows, (h + 1) * hrows)
            prim, tang = norm_pair(inbuf[span, :], probe[span, :].astype(F32), gain_attn[...])
            normed[span, :] = prim
            normed[rows + h * hrows : rows + (h + 1) * hrows, :] = tang

    inbuf[...] = latent[...].astype(F32)
    norm_all()
    for h in range(HALVES):
        state[h] = latent[own_rows(h), :].astype(F32)

    pl.semaphore_wait(barrier, n + m - 2)

    half = cols // 2
    core = lax.rem(s, 2)
    mine = pl.ds(pl.multiple_of(core * half, half), half)
    quarter = half // 2
    turn = lax.rem(s // 2, 2) * (1 - core) + lax.rem(s // 4, 2) * core
    buddy = flip(2) * (1 - core) + flip(4) * core
    fetched = pl.ds(pl.multiple_of(core * half + turn * quarter, quarter), quarter)
    partner = flip(1)
    loads[3].wait()
    w_copies = []
    for d in range(1, m):
        copy = remote(
            wout.at[z, fetched], wout.at[z, fetched], wsend.at[0, d], wrecv.at[0, d], s, zpeer(d)
        )
        copy.start()
        w_copies.append(copy)

    def kv_exchange(k, p):
        bufs = (kbuf, vbuf)
        sends = []

        def give(which, slot, target, at):
            copy = remote(
                bufs[which].at[k, p, slot],
                bufs[which].at[k, p, slot],
                kvsend.at[k, p, len(sends)],
                kvrecv.at[k, p, which, at],
                target,
                z,
            )
            copy.start()
            sends.append(copy)

        def got(which, slot, at):
            pltpu.make_async_copy(
                bufs[which].at[k, p, slot], bufs[which].at[k, p, slot], kvrecv.at[k, p, which, at]
            ).wait()

        xn, yn = flip(2), flip(4)
        dn = yn + 2 - 4 * lax.rem(yn // 2, 2)

        def own(which):
            if n == 8:
                first, second = ((xn, 2), (yn, 4)) if which == 0 else ((yn, 4), (xn, 2))
                give(which, s, *first)
                give(which, s, *second)
                give(which, s, partner, 1)
            else:
                for d in range(1, n):
                    give(which, s, lax.rem(s + d, n), d)

        def relay():
            if n == 8:
                got(0, xn, 2)
                give(0, xn, yn, 6)
                got(1, yn, 4)
                give(1, yn, xn, 6)
                give(0, xn, partner, 3)
                give(1, yn, partner, 5)

        def rest():
            if n == 8:
                got(0, yn, 4)
                give(0, yn, partner, 5)
                got(1, xn, 2)
                give(1, xn, partner, 3)
                got(0, dn, 6)
                give(0, dn, partner, 7)
                got(1, dn, 6)
                give(1, dn, partner, 7)
                slots = ((s, 1), (xn, 3), (yn, 5), (dn, 7))
                for which in range(2):
                    for slot, at in slots:
                        got(which, slot + 1 - 2 * lax.rem(slot, 2), at)
            else:
                for which in range(2):
                    for d in range(1, n):
                        got(which, lax.rem(s + n - d, n), d)

        return sends, own, relay, rest

    lane = lax.broadcasted_iota(jnp.int32, (1, LANES), 1)
    scale = HEAD_DIM ** (-0.5)
    frames = rows * n
    trace = [None] * HALVES

    for k in range(STEPS):

        def project(which):
            if k == 0:
                loads[which].wait()
            weight = wqkv[:, which * cols : (which + 1) * cols]
            return dot(normed[...], weight).astype(BF16).reshape(2, rows, cols)

        def z_start(phase, src_of, dst):
            copies = []
            for d in range(m - 1, 0, -1):
                copy = remote(
                    src_of(zpeer(d)),
                    dst,
                    zsend.at[k, phase, d],
                    zrecv.at[k, phase, d],
                    s,
                    zpeer(d),
                )
                copy.start()
                copies.append(copy)
            return copies

        def z_wait(copies):
            for copy in copies:
                copy.wait_send()
                copy.wait_recv()

        exchanges = [kv_exchange(k, p) for p in range(pairs)]

        def keep_pairs(ref, both):
            for p in range(pairs):
                ref[k, p, s] = both[:, :, p * LANES : (p + 1) * LANES]

        keep_pairs(kbuf, project(1))
        exchanges[0][1](0)
        keep_pairs(vbuf, project(2))
        exchanges[0][1](1)
        qbuf[...] = project(0)
        exchanges[0][2]()
        for p in range(1, pairs):
            exchanges[p][1](0)
            exchanges[p][1](1)
        if k == 0:
            loads[5].wait()
            probe_down[...] = dot_t(probe[...], wdown[...])

        def w_pass(stage, which, target):
            copies = []
            for d in range(1, m):
                copy = remote(
                    wout.at[zfrom(d), which],
                    wout.at[zfrom(d), which],
                    wsend.at[stage, d],
                    wrecv.at[stage, d],
                    target,
                    z,
                )
                copy.start()
                copies.append(copy)
            return copies

        head_copies = [[] for _ in range(HALVES)]
        for p in range(pairs):
            if k == 0 and p == pairs - 1:
                z_wait(w_copies)
                w_trades = w_pass(1, fetched, buddy)
            exchanges[p][3]()
            for h in range(HALVES):
                span = slice(h * hrows, (h + 1) * hrows)
                at = slice(p * LANES, (p + 1) * LANES)
                keys = kbuf[k, p, :, 0].reshape(frames, LANES)
                key_tang = kbuf[k, p, :, 1].reshape(frames, LANES)
                vals = vbuf[k, p, :, 0].reshape(frames, LANES)
                val_tang = vbuf[k, p, :, 1].reshape(frames, LANES)
                both_keys = jnp.concatenate([keys, key_tang], axis=1)
                both_vals = jnp.concatenate([vals, val_tang], axis=1)
                queries = qbuf[0, span, at]
                query_tang = qbuf[1, span, at]
                zero = jnp.zeros_like(queries)
                left = []
                for side in range(LANES // HEAD_DIM):
                    keep = (lane // HEAD_DIM) == side
                    q = jnp.where(keep, queries, zero)
                    qt = jnp.where(keep, query_tang, zero)
                    left.append(
                        (
                            jnp.concatenate([q, zero], axis=1),
                            jnp.concatenate([qt, q], axis=1),
                        )
                    )
                stack = [item[0] for item in left] + [item[1] for item in left]
                both = dot_t(jnp.concatenate(stack, axis=0), both_keys) * scale
                scores, score_tang = both[: 2 * hrows], both[2 * hrows :]
                weights = jnp.exp(scores - jnp.max(scores, axis=-1, keepdims=True))
                weighted = weights * score_tang
                total = jnp.sum(weights, axis=-1, keepdims=True)
                carried = jnp.sum(weighted, axis=-1, keepdims=True)
                rounded = jnp.concatenate([weights.astype(BF16), weighted.astype(BF16)], axis=0)
                mixed = dot(rounded, both_vals)
                prim = mixed[: 2 * hrows, :LANES] / total
                tang = (mixed[2 * hrows :, :LANES] + mixed[: 2 * hrows, LANES:]) / total - (
                    carried / total
                ) * prim
                first = (lane // HEAD_DIM) == 0
                headall[k, h, p, z, 0] = jnp.where(first, prim[:hrows], prim[hrows:]).astype(
                    BF16
                )
                headall[k, h, p, z, 1] = jnp.where(first, tang[:hrows], tang[hrows:]).astype(
                    BF16
                )

                head_copies[h] += z_start(
                    p * HALVES + h, lambda j: headall.at[k, h, p, z], headall.at[k, h, p, z]
                )
                if h == 0 and p + 1 < pairs:
                    exchanges[p + 1][2]()

        if k == 0:
            z_wait(w_trades)
            forwards = w_pass(2, mine, partner)
            loads[4].wait()
            z_wait(forwards)

        rs_copies = []
        for h in range(HALVES):
            span = slice(h * hrows, (h + 1) * hrows)
            z_wait(head_copies[h])
            heads = [
                headall[k, h, p, j].reshape(2 * hrows, LANES) for j in range(m) for p in range(pairs)
            ]
            attn_both = dot(jnp.concatenate(heads, axis=1), wout[...].reshape(m * cols, width))
            attn, attn_tang = attn_both[:hrows], attn_both[hrows:]
            direction = probe[span, :].astype(F32)
            pair = norm_pair(inbuf[span, :] + attn, direction + attn_tang, gain_mlp[...])
            pre = dot(jnp.concatenate(pair, axis=0), win[...])
            act, act_tang = gelu_pair(pre[:hrows], pre[hrows:])
            terms = dot(act, wdown[...])
            rssend[k, h] = terms.astype(BF16).reshape(m, part, width)
            rs_copies.append(
                z_start(pairs * HALVES + h, lambda j: rssend.at[k, h, j], rsrecv.at[k, h, z])
            )
            partial[h] = (attn + terms).reshape(m, part, width)
            grown = jnp.sum(direction * attn_tang, axis=-1, keepdims=True) / m + jnp.sum(
                act_tang.astype(F32) * probe_down[span, :], axis=-1, keepdims=True
            )
            trace[h] = grown if k == 0 else trace[h] + grown

        last = k == STEPS - 1
        if last:
            column = jnp.concatenate(trace, axis=0) / (STEPS * width)
            trace_sum = jnp.sum(column, axis=0, keepdims=True)
            tracebuf[z] = jnp.transpose(jnp.broadcast_to(column, (rows, LANES)))[:8, :]
            trace_copies = []
            for d in range(1, m):
                copy = remote(
                    tracebuf.at[z], tracebuf.at[z], ssend.at[0, d], srecv.at[0, d], s, zpeer(d)
                )
                copy.start()
                trace_copies.append(copy)

        delta_copies = []
        squares = jnp.zeros((1, 1), F32)
        for h in range(HALVES):
            z_wait(rs_copies[h])
            field = partial[h, z]
            for d in range(1, m):
                field = field + rsrecv[k, h, zfrom(d)].astype(F32)
            new_state = state[h] + field / STEPS
            state[h] = new_state
            delta[k, h, z] = (new_state - latent[own_rows(h), :].astype(F32)).astype(BF16)
            delta_copies.append(
                z_start((pairs + 1) * HALVES + h, lambda j: delta.at[k, h, z], delta.at[k, h, z])
            )
            if last:
                by_row = jnp.sum(new_state * new_state, axis=-1, keepdims=True)
                squares = squares + jnp.sum(by_row, axis=0, keepdims=True)
        for exchange in exchanges:
            for send in exchange[0]:
                send.wait_send()
        if last:
            share = trace_sum - 0.5 * squares / width
            tilebuf[z] = jnp.broadcast_to(share, (8, LANES))
            tile_copies = []
            for d in range(1, m):
                copy = remote(
                    tilebuf.at[z], tilebuf.at[z], ssend.at[1, d], srecv.at[1, d], s, zpeer(d)
                )
                copy.start()
                tile_copies.append(copy)
            z_wait(trace_copies)
            trace_row = jnp.sum(tracebuf[...], axis=0)
            z_wait(tile_copies)
            sumbuf[s] = jnp.sum(tilebuf[...], axis=0)
            mean_copies = []
            for d in range(1, n):
                copy = remote(
                    sumbuf.at[s], sumbuf.at[s], msend.at[d], mrecv.at[d], lax.rem(s + d, n), z
                )
                copy.start()
                mean_copies.append(copy)
        norms = []
        for h in range(HALVES):
            span = slice(h * hrows, (h + 1) * hrows)
            z_wait(delta_copies[h])
            following = latent[span, :].astype(F32) + delta[k, h].reshape(hrows, width).astype(F32)
            if last:
                latent_end[span, :] = following
                norms.append(jnp.sum(following * following, axis=-1, keepdims=True))
            else:
                following = following + ((k + 1) / STEPS) * time_embed[...]
                inbuf[span, :] = following
                prim, tang = norm_pair(following, probe[span, :].astype(F32), gain_attn[...])
                normed[span, :] = prim
                normed[rows + h * hrows : rows + (h + 1) * hrows, :] = tang
    norm_row = jnp.transpose(jnp.broadcast_to(jnp.concatenate(norms, axis=0), (rows, LANES)))[:8]
    half_log = 0.5 * math.log(2.0 * math.pi)
    first_row = lax.broadcasted_iota(jnp.int32, (8, rows), 0) == 0
    stats_out[...] = jnp.where(
        first_row, trace_row, trace_row - 0.5 * norm_row / width - half_log
    )
    z_wait(mean_copies)
    mean_out[...] = jnp.sum(sumbuf[...], axis=0) / frames - half_log


def per_device(
    n,
    m,
    latent,
    probe,
    time_embed,
    gain_attn,
    w_query,
    w_key,
    w_value,
    w_out,
    gain_mlp,
    w_in,
    w_down,
):
    rows, width = latent.shape
    cols = w_query.shape[1]
    hidden = w_in.shape[1]
    hrows = rows // HALVES
    part = hrows // m
    pairs = cols // LANES
    vmem = pl.BlockSpec(memory_space=pltpu.VMEM)
    anyspace = pl.BlockSpec(memory_space=pl.ANY)
    dma = pltpu.SemaphoreType.DMA
    state, stats, mean = pl.pallas_call(
        functools.partial(flow_kernel, n, m),
        out_shape=(
            jax.ShapeDtypeStruct((rows, width), F32),
            jax.ShapeDtypeStruct((8, rows), F32),
            jax.ShapeDtypeStruct((8, LANES), F32),
        ),
        in_specs=[vmem] * 5 + [anyspace] * 6,
        out_specs=(vmem, vmem, vmem),
        scratch_shapes=[
            pltpu.VMEM((width, 3 * cols), BF16),
            pltpu.VMEM((m, cols, width), BF16),
            pltpu.VMEM((width, hidden), BF16),
            pltpu.VMEM((hidden, width), BF16),
            pltpu.VMEM((2 * rows, width), BF16),
            pltpu.VMEM((2, rows, cols), BF16),
            pltpu.VMEM((STEPS, pairs, n, 2, rows, LANES), BF16),
            pltpu.VMEM((STEPS, pairs, n, 2, rows, LANES), BF16),
            pltpu.VMEM((STEPS, HALVES, pairs, m, 2, hrows, LANES), BF16),
            pltpu.VMEM((rows, width), F32),
            pltpu.VMEM((rows, hidden), F32),
            pltpu.VMEM((HALVES, m, part, width), F32),
            pltpu.VMEM((STEPS, HALVES, m, part, width), BF16),
            pltpu.VMEM((STEPS, HALVES, m, part, width), BF16),
            pltpu.VMEM((HALVES, part, width), F32),
            pltpu.VMEM((STEPS, HALVES, m, part, width), BF16),
            pltpu.VMEM((m, 8, rows), F32),
            pltpu.VMEM((m, 8, LANES), F32),
            pltpu.VMEM((n, 8, LANES), F32),
            dma((6,)),
            dma((3, m)),
            dma((3, m)),
            dma((STEPS, pairs, 2 * n)),
            dma((STEPS, pairs, 2, n)),
            dma((STEPS, (pairs + 2) * HALVES, m)),
            dma((STEPS, (pairs + 2) * HALVES, m)),
            dma((2, m)),
            dma((2, m)),
            dma((n,)),
            dma((n,)),
        ],
        compiler_params=pltpu.CompilerParams(
            collective_id=0, has_side_effects=True, vmem_limit_bytes=60 * 1024 * 1024
        ),
    )(
        latent,
        probe,
        time_embed.reshape(1, width),
        gain_attn.reshape(1, width),
        gain_mlp.reshape(1, width),
        w_query,
        w_key,
        w_value,
        w_out,
        w_in,
        w_down,
    )
    return (state, stats[0], stats[1], mean[0, 0])


def solution(mesh):
    return jax.shard_map(
        functools.partial(per_device, mesh.shape["seq"], mesh.shape["head"]),
        mesh=mesh,
        in_specs=(
            P("seq", None),
            P("seq", None),
            P(),
            P(),
            P(None, "head"),
            P(None, "head"),
            P(None, "head"),
            P("head", None),
            P(),
            P(None, "head"),
            P("head", None),
        ),
        out_specs=(P("seq", None), P("seq"), P("seq"), P()),
        check_vma=False,
    )
```
